128 devices in a mesh: head: 16 (over z, y_lo, core), kv: 8 (over x, y_hi).
Axes of the slice: x: 4, y: 4 (y_hi: 2, y_lo: 2; y = y_hi * 2 + y_lo), z: 4, core: 2. Of those that a mesh axis runs over, the one named last changes fastest.
Arguments:
- queries: bfloat16 [8192, 8192], P(('kv', 'head')), may hold values from -6 to 6
- key_rows: bfloat16 [8192, 1024], P(('kv', 'head')), may hold values from -6 to 6
- value_matrix: bfloat16 [8192, 1024], P(('kv', 'head')), may hold values from -6 to 6
- doc_ids: int32 [8192], P(('kv', 'head')), may hold values from 0 to 5, as said below
Outputs:
- attended: bfloat16 [8192, 8192], P(('kv', 'head'))
The draws below stay inside these ranges and needn't reach their ends.
Inputs may be any that keep to these rules, and one draw needn't show every extreme that they name: doc_ids starts at 0, never falls, and rises by one at the first token of each of the 6 documents; every document starts at an even position and has 2 tokens or more.
All inputs are finite; a program needn't handle non-finite values.
Results may differ from the reference program's by a relative error of at most 0.015.
Values may be sent and summed in bfloat16 or wider, within the bound.
A program may use at most 64 MiB of HBM per device.

```python
import math
import jax
import jax.numpy as jnp
from jax import lax

QUERY_HEADS = 64
KEY_VALUE_HEADS = 8
HEAD_SIZE = 128
DOCS = 6
SEQUENCE_TOKENS = 8192


def draw_queries(key, part):
    column_total = QUERY_HEADS * HEAD_SIZE
    drawn_values = jax.random.truncated_normal(jax.random.fold_in(key, 1), -6.0, 6.0, (SEQUENCE_TOKENS, column_total), jnp.float32)
    return drawn_values.astype(jnp.bfloat16)


def draw_key_rows(key, part):
    column_total = KEY_VALUE_HEADS * HEAD_SIZE
    drawn_values = jax.random.truncated_normal(jax.random.fold_in(key, 2), -6.0, 6.0, (SEQUENCE_TOKENS, column_total), jnp.float32)
    return drawn_values.astype(jnp.bfloat16)


def draw_doc_ids(key, part):
    pair_count = SEQUENCE_TOKENS // 2
    shuffled = jax.random.permutation(jax.random.fold_in(key, 11), pair_count - 1) + 1
    boundaries = 2 * shuffled[:DOCS - 1]
    positions = jnp.arange(SEQUENCE_TOKENS, dtype=jnp.int32)
    return jnp.sum((positions[:, None] >= boundaries[None, :]).astype(jnp.int32), axis=1).astype(jnp.int32)


def level_of(rng, shape, pieces, smallest, high):
    def one(dim, shards_of):
        draws = jax.random.uniform(jax.random.fold_in(jax.random.fold_in(rng, 6), dim), (shards_of,), jnp.float32, smallest / len(pieces), high / len(pieces))
        return jnp.repeat(jnp.exp(draws), shape[dim] // shards_of).reshape((-1,) + (1,) * (len(shape) - dim - 1))

    factor_of = one(*pieces[0])
    for cut in pieces[1:]:
        factor_of = factor_of * one(*cut)
    return factor_of


def noise(own_key, shape, width, reach, split=(), kind=jnp.bfloat16):
    level = level_of(own_key, shape, split, -0.22, 0.18) if split else 1.0
    drawn = jax.random.normal(own_key, shape, jnp.float32) * width * level
    return jnp.minimum(jnp.maximum(drawn, -reach), reach).astype(kind)


def setup_inputs(seed: int = 0) -> dict:
    splits = jax.random.split(jax.random.key(seed), 5)
    queries = draw_queries(jax.random.fold_in(splits[4], 71), 0)
    key_rows = draw_key_rows(jax.random.fold_in(splits[4], 71), 0)
    value_matrix = noise(splits[2], (SEQUENCE_TOKENS, KEY_VALUE_HEADS * HEAD_SIZE), 1.0, 6.0, ((0, 128),))
    doc_ids = draw_doc_ids(jax.random.fold_in(splits[4], 71), 0)
    return {"queries": queries, "key_rows": key_rows, "value_matrix": value_matrix, "doc_ids": doc_ids}


def reference(queries, key_rows, value_matrix, doc_ids):
    seq_len = queries.shape[0]
    queries_per_group = QUERY_HEADS // KEY_VALUE_HEADS
    block_rows = math.gcd(seq_len, 512)
    scale = HEAD_SIZE ** -0.5

    def single_group(key_value_head):
        head_keys = lax.dynamic_slice_in_dim(key_rows, key_value_head * HEAD_SIZE, HEAD_SIZE, 1).astype(jnp.float32)
        head_values = lax.dynamic_slice_in_dim(value_matrix, key_value_head * HEAD_SIZE, HEAD_SIZE, 1).astype(jnp.float32)
        group_queries = lax.dynamic_slice_in_dim(queries, key_value_head * queries_per_group * HEAD_SIZE, queries_per_group * HEAD_SIZE, 1)
        key_pos = jnp.arange(seq_len, dtype=jnp.int32)

        def one_block(block_index):
            first_row = (block_index * block_rows).astype(jnp.int32)
            rows_now = lax.dynamic_slice_in_dim(group_queries, first_row, block_rows, 0)
            rows_now = rows_now.astype(jnp.float32).reshape(block_rows, queries_per_group, HEAD_SIZE)
            query_pos = first_row + jnp.arange(block_rows, dtype=jnp.int32)
            query_doc = lax.dynamic_slice_in_dim(doc_ids, first_row, block_rows, 0)
            scores = jnp.einsum("rhd,cd->hrc", rows_now, head_keys, precision=lax.Precision.HIGHEST) * scale
            allowed = (key_pos[None, :] <= query_pos[:, None]) & (doc_ids[None, :] == query_doc[:, None])
            masked = jnp.where(allowed, scores, -1.0e30)
            row_max = jnp.max(masked, axis=-1)
            weights = jnp.where(allowed, jnp.exp(masked - row_max[..., None]), 0.0)
            row_sum = jnp.sum(weights, axis=-1)
            rounded = lax.optimization_barrier(weights.astype(jnp.bfloat16)).astype(jnp.float32)
            summed = jnp.einsum("hrc,cd->hrd", rounded, head_values, precision=lax.Precision.HIGHEST)
            result = summed / row_sum[..., None]
            return result.transpose(1, 0, 2).reshape(block_rows, queries_per_group * HEAD_SIZE).astype(jnp.bfloat16)

        blocks = lax.map(one_block, jnp.arange(seq_len // block_rows, dtype=jnp.int32))
        return blocks.reshape(seq_len, queries_per_group * HEAD_SIZE)

    group_total = lax.map(single_group, jnp.arange(KEY_VALUE_HEADS, dtype=jnp.int32))
    return group_total.transpose(1, 0, 2).reshape(seq_len, QUERY_HEADS * HEAD_SIZE)
```

```python
import functools

import jax
import jax.numpy as jnp
from jax import lax
from jax.experimental import pallas as pl
from jax.experimental.pallas import tpu as pltpu
from jax.sharding import PartitionSpec as P

MESH = pl.DeviceIdType.MESH
HEAD_SIZE = 128
GROUP = 8
WIDE = GROUP * HEAD_SIZE
DOCS = 6
TILE = 512
NEG_FILL = -1e30
EXP_SCALE = HEAD_SIZE ** (-0.5) * 1.4426950408889634


def place():
    kv, head = lax.axis_index("kv"), lax.axis_index("head")
    x, z, c = kv // 2, head // 4, head % 2
    y = (kv % 2) * 2 + (head // 2) % 2
    return jnp.where(c == 1, x, y), jnp.where(c == 1, y, x), z, c


def device(a, p, r, c, own_c):
    x = jnp.where(own_c == 1, a, p)
    y = jnp.where(own_c == 1, p, a)
    return {"kv": x * 2 + y // 2, "head": r * 4 + (y % 2) * 2 + c}


def gather_kernel(q_ref, k_ref, v_ref, d_ref, qo, ko, vo, do, lsem, qs, qr, ks, kr, vs, vr, ds, dr,
                  ags, agr, dgs, dgr):
    a, p, r, c = place()
    o = 1 - c
    dev = functools.partial(device, own_c=c)
    up = lambda i, n=1: (i + n) % 4

    barrier = pltpu.get_barrier_semaphore()
    peers = [dev(up(a, n), p, r, c) for n in (1, 2, 3)]
    peers += [dev(a, up(p, n), r, o) for n in range(4)]
    peers += [dev(up(a, n), p, r, o) for n in (1, 2, 3)]
    peers += [dev(a, up(p, n), r, c) for n in (1, 2, 3)]
    peers += [dev(a, p, up(r, n), c) for n in (1, 2, 3)]
    for peer in peers:
        pl.semaphore_signal(barrier, inc=1, device_id=peer, device_id_type=MESH)
    pl.semaphore_wait(barrier, len(peers))

    def rcopy(src, dst, ss, rs, to):
        return pltpu.make_async_remote_copy(
            src_ref=src, dst_ref=dst, send_sem=ss, recv_sem=rs, device_id=to, device_id_type=MESH)

    def cols(ref, g, width):
        return ref.at[:, pl.ds(pl.multiple_of(g * width, width), width)]

    sends = []
    locals_ = []
    g_own = c * 4 + a
    s_own = 2 * a + c
    for i, (src, dst) in enumerate((
        (cols(k_ref, g_own, HEAD_SIZE), ko.at[p, r, s_own]),
        (cols(v_ref, g_own, HEAD_SIZE), vo.at[p, r, s_own]),
        (d_ref, do.at[p, r, s_own]),
        (cols(q_ref, g_own, WIDE), qo.at[s_own]),
    )):
        copy = pltpu.make_async_copy(src, dst, lsem.at[i])
        copy.start()
        locals_.append(copy)

    routes = []
    for n in (1, 3, 2):
        routes.append((0, n, dev(up(a, n), p, r, c), c * 4 + up(a, n), p, 2 * a + c))
    for n in (0, 1, 3, 2):
        routes.append((1, n, dev(a, up(p, n), r, o), o * 4 + up(p, n), a, 2 * p + c))
    for side, n, to, g, pd, sd in routes:
        i = side * 4 + n
        for src, dst, ss, rs in (
            (cols(k_ref, g, HEAD_SIZE), ko.at[pd, r, sd], ks, kr),
            (cols(v_ref, g, HEAD_SIZE), vo.at[pd, r, sd], vs, vr),
            (d_ref, do.at[pd, r, sd], ds, dr),
        ):
            copy = rcopy(src, dst, ss.at[i], rs.at[i], to)
            copy.start()
            sends.append(copy)
    for side, n, to, g, pd, sd in routes:
        i = side * 4 + n
        copy = rcopy(cols(q_ref, g, WIDE), qo.at[sd], qs.at[i], qr.at[i], to)
        copy.start()
        sends.append(copy)

    def landed(ref, sem):
        pltpu.make_async_copy(ref, ref, sem).wait()

    def arrivals(refs):
        for side in (0, 1):
            for n in range(4):
                if (side, n) == (0, 0):
                    continue
                s = 2 * up(a, 4 - n) + (c if side == 0 else o)
                for ref, sem in refs:
                    landed(ref.at[s], sem.at[side * 4 + n])

    for copy in locals_[:3]:
        copy.wait()
    arrivals(((ko.at[p, r], kr), (vo.at[p, r], vr), (do.at[p, r], dr)))

    plus_p, minus_p = dev(a, up(p), r, c), dev(a, up(p, 3), r, c)
    plus_r, minus_r = dev(a, p, up(r), c), dev(a, p, up(r, 3), c)

    def ring(ref, base, at, me, plus, minus):
        blk = lambda i: at(ref, i)
        lo = lambda w: w.at[pl.ds(0, 4)]
        hi = lambda w: w.at[pl.ds(4, 4)]

        def start(src, k, to):
            copy = rcopy(src, src, ags.at[base + k], agr.at[base + k], to)
            copy.start()
            sends.append(copy)

        def first():
            start(blk(me), 0, plus)
            start(blk(me), 1, minus)

        def near():
            landed(blk(up(me, 3)), agr.at[base])
            start(lo(blk(up(me, 3))), 2, plus)
            landed(blk(up(me, 1)), agr.at[base + 1])
            start(hi(blk(up(me, 1))), 3, minus)

        def far():
            landed(lo(blk(up(me, 2))), agr.at[base + 2])
            landed(hi(blk(up(me, 2))), agr.at[base + 3])

        return first, near, far

    def p_ring(ref, base, ri):
        return ring(ref, base, lambda w, i: w.at[i, ri], p, plus_p, minus_p)

    def r_ring(ref, base, pi):
        return ring(ref, base, lambda w, i: w.at[pi, i], r, plus_r, minus_r)

    kp = p_ring(ko, 0, r)
    vr_ = r_ring(vo, 4, p)
    order = (0, 3, 1, 2)
    krs = [r_ring(ko, 8 + 4 * i, up(p, n)) for i, n in enumerate(order)]
    vps = [p_ring(vo, 24 + 4 * i, up(r, n)) for i, n in enumerate(order)]
    kp[0]()
    vr_[0]()
    krs[0][0]()
    vps[0][0]()
    dsend = []
    for n in (1, 2, 3):
        copy = rcopy(do.at[p, r], do.at[p, r], dgs.at[n], dgr.at[n], dev(a, up(p, n), r, c))
        copy.start()
        sends.append(copy)
    kp[1]()
    vr_[1]()
    for i in (1, 2):
        krs[i][0]()
        vps[i][0]()
    krs[0][1]()
    vps[0][1]()
    kp[2]()
    vr_[2]()
    krs[3][0]()
    vps[3][0]()
    for n in (1, 2, 3):
        landed(do.at[up(p, 4 - n), r], dgr.at[n])
    for n in (1, 2, 3):
        copy = rcopy(do.at[:, r], do.at[:, r], dgs.at[3 + n], dgr.at[3 + n], dev(a, p, up(r, n), c))
        copy.start()
        sends.append(copy)
    for i in (1, 2, 3):
        krs[i][1]()
        vps[i][1]()
    for i in range(4):
        krs[i][2]()
        vps[i][2]()
    for n in (1, 2, 3):
        landed(do.at[:, up(r, 4 - n)], dgr.at[3 + n])
    locals_[3].wait()
    arrivals(((qo, qr),))
    for copy in sends:
        copy.wait_send()


def return_kernel(o_ref, out, lsem, ss, rs):
    a, p, r, c = place()
    o = 1 - c
    dev = functools.partial(device, own_c=c)
    up = lambda i, n=1: (i + n) % 4
    barrier = pltpu.get_barrier_semaphore()
    peers = [dev(up(a, n), p, r, c) for n in (1, 2, 3)]
    peers += [dev(a, up(p, n), r, o) for n in range(4)]
    peers += [dev(up(a, n), p, r, o) for n in (1, 2, 3)]
    for peer in peers:
        pl.semaphore_signal(barrier, inc=1, device_id=peer, device_id_type=MESH)
    pl.semaphore_wait(barrier, len(peers))

    def cols(g):
        return out.at[:, pl.ds(pl.multiple_of(g * WIDE, WIDE), WIDE)]

    g_own = c * 4 + a
    own = pltpu.make_async_copy(o_ref.at[2 * a + c], cols(g_own), lsem)
    own.start()
    sends = []
    routes = [(0, n, dev(up(a, n), p, r, c), 2 * up(a, n) + c) for n in (2, 1, 3)]
    routes += [(1, n, dev(up(a, n), p, r, o), 2 * up(a, n) + o) for n in (2, 1, 3, 0)]
    for side, n, to, s in routes:
        i = side * 4 + n
        copy = pltpu.make_async_remote_copy(
            src_ref=o_ref.at[s], dst_ref=cols(g_own), send_sem=ss.at[i], recv_sem=rs.at[i],
            device_id=to, device_id_type=MESH)
        copy.start()
        sends.append(copy)
    own.wait()
    for side, n, to, s in routes:
        i = side * 4 + n
        g = c * 4 + up(a, 4 - n) if side == 0 else o * 4 + up(p, 4 - n)
        pltpu.make_async_copy(cols(g), cols(g), rs.at[i]).wait()
    for copy in sends:
        copy.wait_send()


def attend_kernel(q_ref, k_ref, v_ref, d_ref, o_ref, starts, m_ref, l_ref, acc_ref):
    a, p, r, c = place()
    ch = pl.program_id(0)

    @pl.when(ch == 0)
    def _():
        docs = d_ref[...]
        for t in range(1, DOCS):
            starts[t] = jnp.sum((docs < t).astype(jnp.int32))

    x = jnp.where(c == 1, ch, p)
    y = jnp.where(c == 1, p, ch)
    pos = (x * 16 + (y // 2) * 8 + r * 2 + y % 2) * 128
    first_start = jnp.int32(0)
    last_start = jnp.int32(0)
    row_pos = pos + lax.broadcasted_iota(jnp.int32, (128, 1), 0)
    row_start = jnp.zeros((128, 1), jnp.int32)
    for t in range(1, DOCS):
        st = starts[t]
        first_start = jnp.where(st <= pos, jnp.maximum(first_start, st), first_start)
        last_start = jnp.where(st <= pos + 127, jnp.maximum(last_start, st), last_start)
        row_start = jnp.where(row_pos >= st, jnp.maximum(row_start, st), row_start)

    m_ref[...] = jnp.full(m_ref.shape, NEG_FILL, jnp.float32)
    l_ref[...] = jnp.zeros(l_ref.shape, jnp.float32)
    acc_ref[...] = jnp.zeros(acc_ref.shape, jnp.float32)

    def tile(j, masked):
        ks, vs = [], []
        for i in range(TILE // 128):
            cc = j * (TILE // 128) + i
            tx, ty, tz = cc // 16, (cc // 8) % 2 * 2 + cc % 2, (cc // 2) % 4
            pi = jnp.where(c == 1, ty, tx)
            si = 2 * jnp.where(c == 1, tx, ty)
            ks.append(k_ref[pi, tz, pl.ds(si, 2)].reshape(128, HEAD_SIZE))
            vs.append(v_ref[pi, tz, pl.ds(si, 2)].reshape(128, HEAD_SIZE))
        k = jnp.concatenate(ks, axis=0)
        v = jnp.concatenate(vs, axis=0)
        if masked:
            key = j * TILE + lax.broadcasted_iota(jnp.int32, (128, TILE), 1)
            allowed = (key <= row_pos) & (key >= row_start)
        for h in range(GROUP):
            q = q_ref[:, :, h * HEAD_SIZE:(h + 1) * HEAD_SIZE].reshape(128, HEAD_SIZE)
            s = lax.dot_general(q, k, (((1,), (1,)), ((), ())), preferred_element_type=jnp.float32)
            if masked:
                s = jnp.where(allowed, s, NEG_FILL)
            m_old = m_ref[h]
            m_new = jnp.maximum(m_old, jnp.max(s, axis=1, keepdims=True))
            m_ref[h] = m_new
            alpha = jnp.exp2((m_old - m_new) * EXP_SCALE)
            shift = m_new * EXP_SCALE
            w = [jnp.exp2(s[:, i * 128:(i + 1) * 128] * EXP_SCALE - shift) for i in range(TILE // 128)]
            l_ref[h] = alpha * l_ref[h] + functools.reduce(jnp.add, w)
            weights = jnp.concatenate([t.astype(jnp.bfloat16) for t in w], axis=1)
            acc_ref[h] = alpha * acc_ref[h] + lax.dot_general(
                weights, v, (((1,), (0,)), ((), ())), preferred_element_type=jnp.float32)

    lo = first_start // TILE
    end = (pos + 127) // TILE + 1
    mid_hi = pos // TILE
    mid_lo = jnp.minimum((last_start + TILE - 1) // TILE, mid_hi)

    def run(first, last, masked):
        def body(j, carry):
            tile(j, masked)
            return carry
        lax.fori_loop(first, last, body, 0)

    run(lo, mid_lo, True)
    run(mid_lo, mid_hi, False)
    run(mid_hi, end, True)

    for h in range(GROUP):
        total = jnp.sum(l_ref[h], axis=1, keepdims=True)
        o_ref[:, :, h * HEAD_SIZE:(h + 1) * HEAD_SIZE] = (
            (acc_ref[h] / total).astype(jnp.bfloat16).reshape(2, 64, HEAD_SIZE))


def local(queries, key_rows, value_matrix, doc_ids):
    rows = queries.shape[0]
    docs = jnp.pad(doc_ids, (0, 128 - rows), constant_values=DOCS + 1).reshape(1, 128)
    hbm = pl.BlockSpec(memory_space=pl.ANY)
    dma = pltpu.SemaphoreType.DMA
    q, k, v, d = pl.pallas_call(
        gather_kernel,
        name="gather",
        out_shape=[
            jax.ShapeDtypeStruct((8, rows, WIDE), jnp.bfloat16),
            jax.ShapeDtypeStruct((4, 4, 8, rows, HEAD_SIZE), jnp.bfloat16),
            jax.ShapeDtypeStruct((4, 4, 8, rows, HEAD_SIZE), jnp.bfloat16),
            jax.ShapeDtypeStruct((4, 4, 8, 1, 128), jnp.int32),
        ],
        in_specs=[hbm] * 4,
        out_specs=[hbm] * 4,
        scratch_shapes=[dma((4,))] + [dma((8,))] * 8 + [dma((40,))] * 2 + [dma((7,))] * 2,
        compiler_params=pltpu.CompilerParams(collective_id=0, has_side_effects=True),
    )(queries, key_rows, value_matrix, docs)
    whole = lambda w: pl.BlockSpec(w.shape, lambda i: (0,) * w.ndim)
    chunk = pl.BlockSpec((2, rows, WIDE), lambda i: (i, 0, 0))
    attended = pl.pallas_call(
        attend_kernel,
        name="attend",
        grid=(4,),
        out_shape=jax.ShapeDtypeStruct((8, rows, WIDE), jnp.bfloat16),
        in_specs=[chunk, whole(k), whole(v), whole(d)],
        out_specs=chunk,
        scratch_shapes=[pltpu.SMEM((8,), jnp.int32)] + [pltpu.VMEM((GROUP, 128, 128), jnp.float32)] * 3,
        compiler_params=pltpu.CompilerParams(dimension_semantics=("arbitrary",)),
    )(q, k, v, d)
    return pl.pallas_call(
        return_kernel,
        name="give_back",
        out_shape=jax.ShapeDtypeStruct((rows, 8 * WIDE), jnp.bfloat16),
        in_specs=[hbm],
        out_specs=hbm,
        scratch_shapes=[dma(()), dma((8,)), dma((8,))],
        compiler_params=pltpu.CompilerParams(collective_id=1, has_side_effects=True),
    )(attended)


def solution(mesh):
    tokens = ("kv", "head")
    return jax.shard_map(
        local,
        mesh=mesh,
        in_specs=(P(tokens, None), P(tokens, None), P(tokens, None), P(tokens)),
        out_specs=P(tokens, None),
        check_vma=False,
    )
```

```python
import functools

import jax
import jax.numpy as jnp
from jax import lax
from jax.experimental import pallas as pl
from jax.experimental.pallas import tpu as pltpu
from jax.sharding import PartitionSpec as P

MESH = pl.DeviceIdType.MESH
HEAD_SIZE = 128
GROUP = 8
WIDE = GROUP * HEAD_SIZE
DOCS = 6
TILE = 512
PACK = 2
NEG_FILL = -1e30
EXP_SCALE = HEAD_SIZE ** (-0.5) * 1.4426950408889634


def place():
    kv, head = lax.axis_index("kv"), lax.axis_index("head")
    x, z, c = kv // 2, head // 4, head % 2
    y = (kv % 2) * 2 + (head // 2) % 2
    return jnp.where(c == 1, x, y), jnp.where(c == 1, y, x), z, c


def device(a, p, r, c, own_c):
    x = jnp.where(own_c == 1, a, p)
    y = jnp.where(own_c == 1, p, a)
    return {"kv": x * 2 + y // 2, "head": r * 4 + (y % 2) * 2 + c}


def gather_kernel(q_ref, k_ref, v_ref, d_ref, qo, ko, vo, do, lsem, qs, qr, ks, kr, vs, vr, ds, dr,
                  ags, agr, dgs, dgr):
    a, p, r, c = place()
    o = 1 - c
    dev = functools.partial(device, own_c=c)
    up = lambda i, n=1: (i + n) % 4

    barrier = pltpu.get_barrier_semaphore()
    peers = [dev(up(a, n), p, r, c) for n in (1, 2, 3)]
    peers += [dev(a, up(p, n), r, o) for n in range(4)]
    peers += [dev(up(a, n), p, r, o) for n in (1, 2, 3)]
    peers += [dev(a, up(p, n), r, c) for n in (1, 2, 3)]
    peers += [dev(a, p, up(r, n), c) for n in (1, 2, 3)]
    for peer in peers:
        pl.semaphore_signal(barrier, inc=1, device_id=peer, device_id_type=MESH)
    pl.semaphore_wait(barrier, len(peers))

    def rcopy(src, dst, ss, rs, to):
        return pltpu.make_async_remote_copy(
            src_ref=src, dst_ref=dst, send_sem=ss, recv_sem=rs, device_id=to, device_id_type=MESH)

    def cols(ref, g, width):
        return ref.at[:, pl.ds(pl.multiple_of(g * width, width), width)]

    sends = []
    locals_ = []
    g_own = c * 4 + a
    s_own = 2 * a + c
    for i, (src, dst) in enumerate((
        (cols(k_ref, g_own, HEAD_SIZE), ko.at[p, r, s_own]),
        (cols(v_ref, g_own, HEAD_SIZE), vo.at[p, r, s_own]),
        (d_ref, do.at[p, r, s_own]),
        (cols(q_ref, g_own, WIDE), qo.at[s_own]),
    )):
        copy = pltpu.make_async_copy(src, dst, lsem.at[i])
        copy.start()
        locals_.append(copy)

    routes = []
    for n in (1, 3, 2):
        routes.append((0, n, dev(up(a, n), p, r, c), c * 4 + up(a, n), p, 2 * a + c))
    for n in (0, 1, 3, 2):
        routes.append((1, n, dev(a, up(p, n), r, o), o * 4 + up(p, n), a, 2 * p + c))
    for side, n, to, g, pd, sd in routes:
        i = side * 4 + n
        for src, dst, ss, rs in (
            (cols(k_ref, g, HEAD_SIZE), ko.at[pd, r, sd], ks, kr),
            (cols(v_ref, g, HEAD_SIZE), vo.at[pd, r, sd], vs, vr),
            (d_ref, do.at[pd, r, sd], ds, dr),
        ):
            copy = rcopy(src, dst, ss.at[i], rs.at[i], to)
            copy.start()
            sends.append(copy)
    for side, n, to, g, pd, sd in routes:
        i = side * 4 + n
        copy = rcopy(cols(q_ref, g, WIDE), qo.at[sd], qs.at[i], qr.at[i], to)
        copy.start()
        sends.append(copy)

    def landed(ref, sem):
        pltpu.make_async_copy(ref, ref, sem).wait()

    def arrivals(refs):
        for side in (0, 1):
            for n in range(4):
                if (side, n) == (0, 0):
                    continue
                s = 2 * up(a, 4 - n) + (c if side == 0 else o)
                for ref, sem in refs:
                    landed(ref.at[s], sem.at[side * 4 + n])

    for copy in locals_[:3]:
        copy.wait()
    arrivals(((ko.at[p, r], kr), (vo.at[p, r], vr), (do.at[p, r], dr)))

    plus_p, minus_p = dev(a, up(p), r, c), dev(a, up(p, 3), r, c)
    plus_r, minus_r = dev(a, p, up(r), c), dev(a, p, up(r, 3), c)

    def ring(ref, base, at, me, plus, minus):
        blk = lambda i: at(ref, i)
        lo = lambda w: w.at[pl.ds(0, 4)]
        hi = lambda w: w.at[pl.ds(4, 4)]

        def start(src, k, to):
            copy = rcopy(src, src, ags.at[base + k], agr.at[base + k], to)
            copy.start()
            sends.append(copy)

        def first():
            start(blk(me), 0, plus)
            start(blk(me), 1, minus)

        def near():
            landed(blk(up(me, 3)), agr.at[base])
            start(lo(blk(up(me, 3))), 2, plus)
            landed(blk(up(me, 1)), agr.at[base + 1])
            start(hi(blk(up(me, 1))), 3, minus)

        def far():
            landed(lo(blk(up(me, 2))), agr.at[base + 2])
            landed(hi(blk(up(me, 2))), agr.at[base + 3])

        return first, near, far

    def p_ring(ref, base, ri):
        return ring(ref, base, lambda w, i: w.at[i, ri], p, plus_p, minus_p)

    def r_ring(ref, base, pi):
        return ring(ref, base, lambda w, i: w.at[pi, i], r, plus_r, minus_r)

    kp = p_ring(ko, 0, r)
    vr_ = r_ring(vo, 4, p)
    order = (0, 3, 1, 2)
    krs = [r_ring(ko, 8 + 4 * i, up(p, n)) for i, n in enumerate(order)]
    vps = [p_ring(vo, 24 + 4 * i, up(r, n)) for i, n in enumerate(order)]
    kp[0]()
    vr_[0]()
    krs[0][0]()
    vps[0][0]()
    dsend = []
    for n in (1, 2, 3):
        copy = rcopy(do.at[p, r], do.at[p, r], dgs.at[n], dgr.at[n], dev(a, up(p, n), r, c))
        copy.start()
        sends.append(copy)
    kp[1]()
    vr_[1]()
    for i in (1, 2):
        krs[i][0]()
        vps[i][0]()
    krs[0][1]()
    vps[0][1]()
    kp[2]()
    vr_[2]()
    krs[3][0]()
    vps[3][0]()
    for n in (1, 2, 3):
        landed(do.at[up(p, 4 - n), r], dgr.at[n])
    for n in (1, 2, 3):
        copy = rcopy(do.at[:, r], do.at[:, r], dgs.at[3 + n], dgr.at[3 + n], dev(a, p, up(r, n), c))
        copy.start()
        sends.append(copy)
    for i in (1, 2, 3):
        krs[i][1]()
        vps[i][1]()
    for i in range(4):
        krs[i][2]()
        vps[i][2]()
    for n in (1, 2, 3):
        landed(do.at[:, up(r, 4 - n)], dgr.at[3 + n])
    locals_[3].wait()
    arrivals(((qo, qr),))
    for copy in sends:
        copy.wait_send()


def return_kernel(o_ref, out, lsem, ss, rs):
    a, p, r, c = place()
    o = 1 - c
    dev = functools.partial(device, own_c=c)
    up = lambda i, n=1: (i + n) % 4
    barrier = pltpu.get_barrier_semaphore()
    peers = [dev(up(a, n), p, r, c) for n in (1, 2, 3)]
    peers += [dev(a, up(p, n), r, o) for n in range(4)]
    peers += [dev(up(a, n), p, r, o) for n in (1, 2, 3)]
    for peer in peers:
        pl.semaphore_signal(barrier, inc=1, device_id=peer, device_id_type=MESH)
    pl.semaphore_wait(barrier, len(peers))

    def cols(g):
        return out.at[:, pl.ds(pl.multiple_of(g * WIDE, WIDE), WIDE)]

    g_own = c * 4 + a
    own = pltpu.make_async_copy(o_ref.at[2 * a + c], cols(g_own), lsem)
    own.start()
    sends = []
    routes = [(0, n, dev(up(a, n), p, r, c), 2 * up(a, n) + c) for n in (2, 1, 3)]
    routes += [(1, n, dev(up(a, n), p, r, o), 2 * up(a, n) + o) for n in (2, 1, 3, 0)]
    for side, n, to, s in routes:
        i = side * 4 + n
        copy = pltpu.make_async_remote_copy(
            src_ref=o_ref.at[s], dst_ref=cols(g_own), send_sem=ss.at[i], recv_sem=rs.at[i],
            device_id=to, device_id_type=MESH)
        copy.start()
        sends.append(copy)
    own.wait()
    for side, n, to, s in routes:
        i = side * 4 + n
        g = c * 4 + up(a, 4 - n) if side == 0 else o * 4 + up(p, 4 - n)
        pltpu.make_async_copy(cols(g), cols(g), rs.at[i]).wait()
    for copy in sends:
        copy.wait_send()


def attend_kernel(q_ref, k_ref, v_ref, d_ref, o_ref, tab, qt_ref, rs_ref, m_ref, acc_ref,
                  s_a, mx_a, w_a, al_a, s_b, mx_b, w_b, al_b):
    a, p, r, c = place()
    lanes = GROUP * 128
    sets = ((s_a, mx_a, w_a, al_a), (s_b, mx_b, w_b, al_b))

    def chunk_pos(ch):
        x = jnp.where(c == 1, ch, p)
        y = jnp.where(c == 1, p, ch)
        return (x * 16 + (y // 2) * 8 + r * 2 + y % 2) * 128

    docs = d_ref[...]
    starts = [jnp.sum((docs < t).astype(jnp.int32)) for t in range(1, DOCS)]
    count = jnp.int32(1)
    for ch in range(4):
        pos = chunk_pos(ch)
        first_start = jnp.int32(0)
        last_start = jnp.int32(0)
        row_pos = pos + lax.broadcasted_iota(jnp.int32, (1, 128), 1)
        row_start = jnp.zeros((1, 128), jnp.int32)
        for st in starts:
            first_start = jnp.where(st <= pos, jnp.maximum(first_start, st), first_start)
            last_start = jnp.where(st <= pos + 127, jnp.maximum(last_start, st), last_start)
            row_start = jnp.where(row_pos >= st, jnp.maximum(row_start, st), row_start)
        rs_ref[ch] = row_start
        lo = first_start // TILE
        end = (pos + 127) // TILE + 1

        def put(j, n):
            tab[0, n] = ch
            tab[1, n] = j
            tab[2, n] = jnp.where((j * TILE < last_start) | (j * TILE + TILE - 1 > pos), 1, 0)
            return n + 1

        count = lax.fori_loop(lo, end, put, count)
        for h in range(GROUP):
            q = q_ref[2 * ch:2 * ch + 2, :, h * HEAD_SIZE:(h + 1) * HEAD_SIZE].reshape(128, HEAD_SIZE)
            qt_ref[ch, :, h * 128:(h + 1) * 128] = q.T
    for i, at in ((0, 0), (1, count), (2, count + 1)):
        tab[0, at] = 0
        tab[1, at] = 0
        tab[2, at] = 0
    steps = count - 1

    m_ref[...] = jnp.full(m_ref.shape, NEG_FILL, jnp.float32)
    acc_ref[...] = jnp.zeros(acc_ref.shape, jnp.float32)
    w_b[...] = jnp.zeros(w_b.shape, jnp.bfloat16)
    al_b[...] = jnp.ones(al_b.shape, jnp.float32)

    def part(j, i):
        cc = j * (TILE // 128) + i
        tx, ty, tz = cc // 16, (cc // 8) % 2 * 2 + cc % 2, (cc // 2) % 4
        return jnp.where(c == 1, ty, tx), tz, pl.ds(2 * jnp.where(c == 1, tx, ty), 2)

    parts = TILE // 128
    span = PACK * 128

    def score(at, masked, to):
        s_ref, mx_ref = to[:2]
        ch, j = tab[0, at], tab[1, at]
        k = jnp.concatenate([k_ref[part(j, i)].reshape(128, HEAD_SIZE) for i in range(parts)], axis=0)
        if masked:
            row_pos = chunk_pos(ch) + lax.broadcasted_iota(jnp.int32, (1, 128), 1)
            key = j * TILE + lax.broadcasted_iota(jnp.int32, (TILE, 128), 0)
            allowed = (key <= row_pos) & (key >= rs_ref[ch])
            allowed = jnp.concatenate([allowed] * PACK, axis=1)

        def group(g):
            cols = slice(g * span, (g + 1) * span)
            s = lax.dot_general(k, qt_ref[ch, :, cols], (((1,), (0,)), ((), ())),
                                preferred_element_type=jnp.float32)
            if masked:
                s = jnp.where(allowed, s, NEG_FILL)
            s_ref[:, cols] = s
            mx_ref[:, cols] = jnp.max(s, axis=0, keepdims=True)
        return group

    def weigh(at, have):
        s_ref, mx_ref, w_ref, al_ref = have
        ch = tab[0, at]

        def group(g):
            cols = slice(g * span, (g + 1) * span)
            m_old = m_ref[ch, :, cols]
            m_new = jnp.maximum(m_old, mx_ref[:, cols])
            m_ref[ch, :, cols] = m_new
            al_ref[:, cols] = jnp.exp2((m_old - m_new) * EXP_SCALE)
            w_ref[:, cols] = jnp.exp2(s_ref[:, cols] * EXP_SCALE - m_new * EXP_SCALE).astype(jnp.bfloat16)
        return group

    def gather_values(at, have):
        w_ref, al_ref = have[2:]
        ch, j = tab[0, at], tab[1, at]
        vt = jnp.concatenate([v_ref[part(j, i)].reshape(128, HEAD_SIZE).T for i in range(parts)], axis=1)
        vt = jnp.concatenate([vt, jnp.ones((16, TILE), jnp.bfloat16)], axis=0)

        def group(g):
            cols = slice(g * span, (g + 1) * span)
            acc_ref[ch, :, cols] = al_ref[:, cols] * acc_ref[ch, :, cols] + lax.dot_general(
                vt, w_ref[:, cols], (((1,), (0,)), ((), ())), preferred_element_type=jnp.float32)
        return group

    def step(it, have, other):
        def body(masked):
            stages = (score(it + 2, masked, other), weigh(it + 1, have), gather_values(it, other))
            for g in range(GROUP // PACK):
                for stage in stages:
                    stage(g)

        flag = tab[2, it + 2]

        @pl.when(flag == 1)
        def _():
            body(True)

        @pl.when(flag == 0)
        def _():
            body(False)

    def opening(masked):
        stage = score(1, masked, sets[0])
        for g in range(GROUP // PACK):
            stage(g)

    opening(True)

    def pair(i, carry):
        step(2 * i, sets[0], sets[1])

        @pl.when(2 * i + 1 < steps)
        def _():
            step(2 * i + 1, sets[1], sets[0])
        return carry

    lax.fori_loop(0, (steps + 1) // 2, pair, 0)

    def closing(have):
        stage = gather_values(steps, have)
        for g in range(GROUP // PACK):
            stage(g)

    @pl.when(steps % 2 == 1)
    def _():
        closing(sets[0])

    @pl.when(steps % 2 == 0)
    def _():
        closing(sets[1])

    for ch in range(4):
        for h in range(GROUP):
            cols = slice(h * 128, (h + 1) * 128)
            out = acc_ref[ch, 0:HEAD_SIZE, cols] / acc_ref[ch, HEAD_SIZE:HEAD_SIZE + 1, cols]
            o_ref[2 * ch:2 * ch + 2, :, h * HEAD_SIZE:(h + 1) * HEAD_SIZE] = (
                out.T.astype(jnp.bfloat16).reshape(2, 64, HEAD_SIZE))


def attend(q, k, v, d):
    rows = q.shape[1]
    lanes = GROUP * 128
    f32 = jnp.float32
    stage = [
        pltpu.VMEM((TILE, lanes), f32),
        pltpu.VMEM((1, lanes), f32),
        pltpu.VMEM((TILE, lanes), jnp.bfloat16),
        pltpu.VMEM((1, lanes), f32),
    ]
    return pl.pallas_call(
        attend_kernel,
        name="attend",
        out_shape=jax.ShapeDtypeStruct((8, rows, WIDE), jnp.bfloat16),
        in_specs=[pl.BlockSpec(memory_space=pltpu.VMEM)] * 4,
        out_specs=pl.BlockSpec(memory_space=pltpu.VMEM),
        scratch_shapes=[
            pltpu.SMEM((3, 128), jnp.int32),
            pltpu.VMEM((4, HEAD_SIZE, lanes), jnp.bfloat16),
            pltpu.VMEM((4, 1, 128), jnp.int32),
            pltpu.VMEM((4, 1, lanes), f32),
            pltpu.VMEM((4, HEAD_SIZE + 16, lanes), f32),
        ] + stage + stage,
    )(q, k, v, d)


def local(queries, key_rows, value_matrix, doc_ids):
    rows = queries.shape[0]
    docs = jnp.pad(doc_ids, (0, 128 - rows), constant_values=DOCS + 1).reshape(1, 128)
    hbm = pl.BlockSpec(memory_space=pl.ANY)
    dma = pltpu.SemaphoreType.DMA
    q, k, v, d = pl.pallas_call(
        gather_kernel,
        name="gather",
        out_shape=[
            jax.ShapeDtypeStruct((8, rows, WIDE), jnp.bfloat16),
            jax.ShapeDtypeStruct((4, 4, 8, rows, HEAD_SIZE), jnp.bfloat16),
            jax.ShapeDtypeStruct((4, 4, 8, rows, HEAD_SIZE), jnp.bfloat16),
            jax.ShapeDtypeStruct((4, 4, 8, 1, 128), jnp.int32),
        ],
        in_specs=[hbm] * 4,
        out_specs=[hbm] * 4,
        scratch_shapes=[dma((4,))] + [dma((8,))] * 8 + [dma((40,))] * 2 + [dma((7,))] * 2,
        compiler_params=pltpu.CompilerParams(collective_id=0, has_side_effects=True),
    )(queries, key_rows, value_matrix, docs)
    attended = attend(q, k, v, d)
    return pl.pallas_call(
        return_kernel,
        name="give_back",
        out_shape=jax.ShapeDtypeStruct((rows, 8 * WIDE), jnp.bfloat16),
        in_specs=[hbm],
        out_specs=hbm,
        scratch_shapes=[dma(()), dma((8,)), dma((8,))],
        compiler_params=pltpu.CompilerParams(collective_id=1, has_side_effects=True),
    )(attended)


def solution(mesh):
    tokens = ("kv", "head")
    return jax.shard_map(
        local,
        mesh=mesh,
        in_specs=(P(tokens, None), P(tokens, None), P(tokens, None), P(tokens)),
        out_specs=P(tokens, None),
        check_vma=False,
    )
```

```python
import functools

import jax
import jax.numpy as jnp
from jax import lax
from jax.experimental import pallas as pl
from jax.experimental.pallas import tpu as pltpu
from jax.sharding import PartitionSpec as P

MESH = pl.DeviceIdType.MESH
HEAD_SIZE = 128
GROUP = 8
WIDE = GROUP * HEAD_SIZE
DOCS = 6
TILE = 512
PACK = 2
NEG_FILL = -1e30
EXP_SCALE = HEAD_SIZE ** (-0.5) * 1.4426950408889634


def place():
    kv, head = lax.axis_index("kv"), lax.axis_index("head")
    x, z, c = kv // 2, head // 4, head % 2
    y = (kv % 2) * 2 + (head // 2) % 2
    return jnp.where(c == 1, x, y), jnp.where(c == 1, y, x), z, c


def device(a, p, r, c, own_c):
    x = jnp.where(own_c == 1, a, p)
    y = jnp.where(own_c == 1, p, a)
    return {"kv": x * 2 + y // 2, "head": r * 4 + (y % 2) * 2 + c}


def gather_kernel(q_ref, k_ref, v_ref, d_ref, qo, ko, vo, do, lsem, qs, qr, ks, kr, vs, vr, ds, dr,
                  ags, agr, dgs, dgr):
    a, p, r, c = place()
    o = 1 - c
    dev = functools.partial(device, own_c=c)
    up = lambda i, n=1: (i + n) % 4

    barrier = pltpu.get_barrier_semaphore()
    peers = [dev(up(a, n), p, r, c) for n in (1, 2, 3)]
    peers += [dev(a, up(p, n), r, o) for n in range(4)]
    peers += [dev(up(a, n), p, r, o) for n in (1, 2, 3)]
    peers += [dev(a, up(p, n), r, c) for n in (1, 2, 3)]
    peers += [dev(a, p, up(r, n), c) for n in (1, 2, 3)]
    for peer in peers:
        pl.semaphore_signal(barrier, inc=1, device_id=peer, device_id_type=MESH)
    pl.semaphore_wait(barrier, len(peers))

    def rcopy(src, dst, ss, rs, to):
        return pltpu.make_async_remote_copy(
            src_ref=src, dst_ref=dst, send_sem=ss, recv_sem=rs, device_id=to, device_id_type=MESH)

    def cols(ref, g, width):
        return ref.at[:, pl.ds(pl.multiple_of(g * width, width), width)]

    sends = []
    locals_ = []
    g_own = c * 4 + a
    s_own = 2 * a + c
    for i, (src, dst) in enumerate((
        (cols(k_ref, g_own, HEAD_SIZE), ko.at[p, r, s_own]),
        (cols(v_ref, g_own, HEAD_SIZE), vo.at[p, r, s_own]),
        (d_ref, do.at[p, r, s_own]),
        (cols(q_ref, g_own, WIDE), qo.at[s_own]),
    )):
        copy = pltpu.make_async_copy(src, dst, lsem.at[i])
        copy.start()
        locals_.append(copy)

    routes = []
    for n in (1, 3, 2):
        routes.append((0, n, dev(up(a, n), p, r, c), c * 4 + up(a, n), p, 2 * a + c))
    for n in (0, 1, 3, 2):
        routes.append((1, n, dev(a, up(p, n), r, o), o * 4 + up(p, n), a, 2 * p + c))
    for side, n, to, g, pd, sd in routes:
        i = side * 4 + n
        for src, dst, ss, rs in (
            (cols(k_ref, g, HEAD_SIZE), ko.at[pd, r, sd], ks, kr),
            (cols(v_ref, g, HEAD_SIZE), vo.at[pd, r, sd], vs, vr),
            (d_ref, do.at[pd, r, sd], ds, dr),
        ):
            copy = rcopy(src, dst, ss.at[i], rs.at[i], to)
            copy.start()
            sends.append(copy)
    for side, n, to, g, pd, sd in routes:
        i = side * 4 + n
        copy = rcopy(cols(q_ref, g, WIDE), qo.at[sd], qs.at[i], qr.at[i], to)
        copy.start()
        sends.append(copy)

    def landed(ref, sem):
        pltpu.make_async_copy(ref, ref, sem).wait()

    def arrivals(refs):
        for side in (0, 1):
            for n in range(4):
                if (side, n) == (0, 0):
                    continue
                s = 2 * up(a, 4 - n) + (c if side == 0 else o)
                for ref, sem in refs:
                    landed(ref.at[s], sem.at[side * 4 + n])

    for copy in locals_[:3]:
        copy.wait()
    arrivals(((ko.at[p, r], kr), (vo.at[p, r], vr), (do.at[p, r], dr)))

    plus_p, minus_p = dev(a, up(p), r, c), dev(a, up(p, 3), r, c)
    plus_r, minus_r = dev(a, p, up(r), c), dev(a, p, up(r, 3), c)

    def ring(ref, base, at, me, plus, minus):
        blk = lambda i: at(ref, i)
        lo = lambda w: w.at[pl.ds(0, 4)]
        hi = lambda w: w.at[pl.ds(4, 4)]

        def start(src, k, to):
            copy = rcopy(src, src, ags.at[base + k], agr.at[base + k], to)
            copy.start()
            sends.append(copy)

        def first():
            start(blk(me), 0, plus)
            start(blk(me), 1, minus)

        def near():
            landed(blk(up(me, 3)), agr.at[base])
            start(lo(blk(up(me, 3))), 2, plus)
            landed(blk(up(me, 1)), agr.at[base + 1])
            start(hi(blk(up(me, 1))), 3, minus)

        def far():
            landed(lo(blk(up(me, 2))), agr.at[base + 2])
            landed(hi(blk(up(me, 2))), agr.at[base + 3])

        return first, near, far

    def p_ring(ref, base, ri):
        return ring(ref, base, lambda w, i: w.at[i, ri], p, plus_p, minus_p)

    def r_ring(ref, base, pi):
        return ring(ref, base, lambda w, i: w.at[pi, i], r, plus_r, minus_r)

    kp = p_ring(ko, 0, r)
    vr_ = r_ring(vo, 4, p)
    order = (0, 3, 1, 2)
    krs = [r_ring(ko, 8 + 4 * i, up(p, n)) for i, n in enumerate(order)]
    vps = [p_ring(vo, 24 + 4 * i, up(r, n)) for i, n in enumerate(order)]
    kp[0]()
    vr_[0]()
    krs[0][0]()
    vps[0][0]()
    dsend = []
    for n in (1, 2, 3):
        copy = rcopy(do.at[p, r], do.at[p, r], dgs.at[n], dgr.at[n], dev(a, up(p, n), r, c))
        copy.start()
        sends.append(copy)
    kp[1]()
    vr_[1]()
    for i in (1, 2):
        krs[i][0]()
        vps[i][0]()
    krs[0][1]()
    vps[0][1]()
    kp[2]()
    vr_[2]()
    krs[3][0]()
    vps[3][0]()
    for n in (1, 2, 3):
        landed(do.at[up(p, 4 - n), r], dgr.at[n])
    for n in (1, 2, 3):
        copy = rcopy(do.at[:, r], do.at[:, r], dgs.at[3 + n], dgr.at[3 + n], dev(a, p, up(r, n), c))
        copy.start()
        sends.append(copy)
    for i in (1, 2, 3):
        krs[i][1]()
        vps[i][1]()
    for i in range(4):
        krs[i][2]()
        vps[i][2]()
    for n in (1, 2, 3):
        landed(do.at[:, up(r, 4 - n)], dgr.at[3 + n])
    locals_[3].wait()
    arrivals(((qo, qr),))
    for copy in sends:
        copy.wait_send()


def return_kernel(o_ref, out, lsem, ss, rs):
    a, p, r, c = place()
    o = 1 - c
    dev = functools.partial(device, own_c=c)
    up = lambda i, n=1: (i + n) % 4
    barrier = pltpu.get_barrier_semaphore()
    peers = [dev(up(a, n), p, r, c) for n in (1, 2, 3)]
    peers += [dev(a, up(p, n), r, o) for n in range(4)]
    peers += [dev(up(a, n), p, r, o) for n in (1, 2, 3)]
    for peer in peers:
        pl.semaphore_signal(barrier, inc=1, device_id=peer, device_id_type=MESH)
    pl.semaphore_wait(barrier, len(peers))

    def cols(g):
        return out.at[:, pl.ds(pl.multiple_of(g * WIDE, WIDE), WIDE)]

    g_own = c * 4 + a
    own = pltpu.make_async_copy(o_ref.at[2 * a + c], cols(g_own), lsem)
    own.start()
    sends = []
    routes = [(0, n, dev(up(a, n), p, r, c), 2 * up(a, n) + c) for n in (2, 1, 3)]
    routes += [(1, n, dev(up(a, n), p, r, o), 2 * up(a, n) + o) for n in (2, 1, 3, 0)]
    for side, n, to, s in routes:
        i = side * 4 + n
        copy = pltpu.make_async_remote_copy(
            src_ref=o_ref.at[s], dst_ref=cols(g_own), send_sem=ss.at[i], recv_sem=rs.at[i],
            device_id=to, device_id_type=MESH)
        copy.start()
        sends.append(copy)
    own.wait()
    for side, n, to, s in routes:
        i = side * 4 + n
        g = c * 4 + up(a, 4 - n) if side == 0 else o * 4 + up(p, 4 - n)
        pltpu.make_async_copy(cols(g), cols(g), rs.at[i]).wait()
    for copy in sends:
        copy.wait_send()


def attend_kernel(q_ref, k_ref, v_ref, d_ref, o_ref, tab, qt_ref, rs_ref, m_ref, acc_ref,
                  s_a, mx_a, w_a, al_a, s_b, mx_b, w_b, al_b):
    a, p, r, c = place()
    lanes = GROUP * 128
    sets = ((s_a, mx_a, w_a, al_a), (s_b, mx_b, w_b, al_b))

    def chunk_pos(ch):
        x = jnp.where(c == 1, ch, p)
        y = jnp.where(c == 1, p, ch)
        return (x * 16 + (y // 2) * 8 + r * 2 + y % 2) * 128

    docs = d_ref[...]
    starts = [jnp.sum((docs < t).astype(jnp.int32)) for t in range(1, DOCS)]
    count = jnp.int32(1)
    for ch in range(4):
        pos = chunk_pos(ch)
        first_start = jnp.int32(0)
        last_start = jnp.int32(0)
        row_pos = pos + lax.broadcasted_iota(jnp.int32, (1, 128), 1)
        row_start = jnp.zeros((1, 128), jnp.int32)
        for st in starts:
            first_start = jnp.where(st <= pos, jnp.maximum(first_start, st), first_start)
            last_start = jnp.where(st <= pos + 127, jnp.maximum(last_start, st), last_start)
            row_start = jnp.where(row_pos >= st, jnp.maximum(row_start, st), row_start)
        rs_ref[ch] = row_start
        lo = first_start // TILE
        end = (pos + 127) // TILE + 1

        def put(j, n):
            tab[0, n] = ch
            tab[1, n] = j
            tab[2, n] = jnp.where((j * TILE < last_start) | (j * TILE + TILE - 1 > pos), 1, 0)
            return n + 1

        count = lax.fori_loop(lo, end, put, count)
        for h in range(GROUP):
            q = q_ref[2 * ch:2 * ch + 2, :, h * HEAD_SIZE:(h + 1) * HEAD_SIZE].reshape(128, HEAD_SIZE)
            qt_ref[ch, :, h * 128:(h + 1) * 128] = q.T
    for i, at in ((0, 0), (1, count), (2, count + 1)):
        tab[0, at] = 0
        tab[1, at] = 0
        tab[2, at] = 0
    steps = count - 1

    m_ref[...] = jnp.full(m_ref.shape, NEG_FILL, jnp.float32)
    acc_ref[...] = jnp.zeros(acc_ref.shape, jnp.float32)
    w_b[...] = jnp.zeros(w_b.shape, jnp.bfloat16)
    al_b[...] = jnp.ones(al_b.shape, jnp.float32)

    def part(j, i):
        cc = j * (TILE // 128) + i
        tx, ty, tz = cc // 16, (cc // 8) % 2 * 2 + cc % 2, (cc // 2) % 4
        return jnp.where(c == 1, ty, tx), tz, pl.ds(2 * jnp.where(c == 1, tx, ty), 2)

    parts = TILE // 128
    span = PACK * 128

    def score(at, masked, to):
        s_ref, mx_ref = to[:2]
        ch, j = tab[0, at], tab[1, at]
        k = jnp.concatenate([k_ref[part(j, i)].reshape(128, HEAD_SIZE) for i in range(parts)], axis=0)
        if masked:
            row_pos = chunk_pos(ch) + lax.broadcasted_iota(jnp.int32, (1, 128), 1)
            key = j * TILE + lax.broadcasted_iota(jnp.int32, (TILE, 128), 0)
            allowed = (key <= row_pos) & (key >= rs_ref[ch])
            allowed = jnp.concatenate([allowed] * PACK, axis=1)

        def group(g):
            cols = slice(g * span, (g + 1) * span)
            s = lax.dot_general(k, qt_ref[ch, :, cols], (((1,), (0,)), ((), ())),
                                preferred_element_type=jnp.float32)
            if masked:
                s = jnp.where(allowed, s, NEG_FILL)
            s_ref[:, cols] = s
            mx_ref[:, cols] = jnp.max(s, axis=0, keepdims=True)
        return group

    def weigh(at, have):
        s_ref, mx_ref, w_ref, al_ref = have
        ch = tab[0, at]

        def group(g):
            cols = slice(g * span, (g + 1) * span)
            m_old = m_ref[ch, :, cols]
            m_new = jnp.maximum(m_old, mx_ref[:, cols])
            m_ref[ch, :, cols] = m_new
            al_ref[:, cols] = jnp.exp2((m_old - m_new) * EXP_SCALE)
            w_ref[:, cols] = jnp.exp2(s_ref[:, cols] * EXP_SCALE - m_new * EXP_SCALE).astype(jnp.bfloat16)
        return group

    def gather_values(at, have):
        w_ref, al_ref = have[2:]
        ch, j = tab[0, at], tab[1, at]
        vt = jnp.concatenate([v_ref[part(j, i)].reshape(128, HEAD_SIZE).T for i in range(parts)], axis=1)
        vt = jnp.concatenate([vt, jnp.ones((16, TILE), jnp.bfloat16)], axis=0)

        def group(g):
            cols = slice(g * span, (g + 1) * span)
            acc_ref[ch, :, cols] = al_ref[:, cols] * acc_ref[ch, :, cols] + lax.dot_general(
                vt, w_ref[:, cols], (((1,), (0,)), ((), ())), preferred_element_type=jnp.float32)
        return group

    def step(it, have, other):
        def body(masked):
            stages = (score(it + 2, masked, other), weigh(it + 1, have), gather_values(it, other))
            for g in range(GROUP // PACK):
                for stage in stages:
                    stage(g)

        flag = tab[2, it + 2]

        @pl.when(flag == 1)
        def _():
            body(True)

        @pl.when(flag == 0)
        def _():
            body(False)

    def opening(masked):
        stage = score(1, masked, sets[0])
        for g in range(GROUP // PACK):
            stage(g)

    opening(True)

    def pair(i, carry):
        step(2 * i, sets[0], sets[1])

        @pl.when(2 * i + 1 < steps)
        def _():
            step(2 * i + 1, sets[1], sets[0])
        return carry

    lax.fori_loop(0, (steps + 1) // 2, pair, 0)

    def closing(have):
        stage = gather_values(steps, have)
        for g in range(GROUP // PACK):
            stage(g)

    @pl.when(steps % 2 == 1)
    def _():
        closing(sets[0])

    @pl.when(steps % 2 == 0)
    def _():
        closing(sets[1])

    for ch in range(4):
        for h in range(GROUP):
            cols = slice(h * 128, (h + 1) * 128)
            out = acc_ref[ch, 0:HEAD_SIZE, cols] / acc_ref[ch, HEAD_SIZE:HEAD_SIZE + 1, cols]
            o_ref[2 * ch:2 * ch + 2, :, h * HEAD_SIZE:(h + 1) * HEAD_SIZE] = (
                out.T.astype(jnp.bfloat16).reshape(2, 64, HEAD_SIZE))


def attend(q, k, v, d):
    rows = q.shape[1]
    lanes = GROUP * 128
    f32 = jnp.float32
    stage = [
        pltpu.VMEM((TILE, lanes), f32),
        pltpu.VMEM((1, lanes), f32),
        pltpu.VMEM((TILE, lanes), jnp.bfloat16),
        pltpu.VMEM((1, lanes), f32),
    ]
    return pl.pallas_call(
        attend_kernel,
        name="attend",
        out_shape=jax.ShapeDtypeStruct((8, rows, WIDE), jnp.bfloat16),
        in_specs=[pl.BlockSpec(memory_space=pltpu.VMEM)] * 4,
        out_specs=pl.BlockSpec(memory_space=pltpu.VMEM),
        scratch_shapes=[
            pltpu.SMEM((3, 128), jnp.int32),
            pltpu.VMEM((4, HEAD_SIZE, lanes), jnp.bfloat16),
            pltpu.VMEM((4, 1, 128), jnp.int32),
            pltpu.VMEM((4, 1, lanes), f32),
            pltpu.VMEM((4, HEAD_SIZE + 16, lanes), f32),
        ] + stage + stage,
        compiler_params=pltpu.CompilerParams(vmem_limit_bytes=30 * 2**20),
    )(q, k, v, d)


def local(queries, key_rows, value_matrix, doc_ids):
    rows = queries.shape[0]
    docs = jnp.pad(doc_ids, (0, 128 - rows), constant_values=DOCS + 1).reshape(1, 128)
    hbm = pl.BlockSpec(memory_space=pl.ANY)
    dma = pltpu.SemaphoreType.DMA
    q, k, v, d = pl.pallas_call(
        gather_kernel,
        name="gather",
        out_shape=[
            jax.ShapeDtypeStruct((8, rows, WIDE), jnp.bfloat16),
            jax.ShapeDtypeStruct((4, 4, 8, rows, HEAD_SIZE), jnp.bfloat16),
            jax.ShapeDtypeStruct((4, 4, 8, rows, HEAD_SIZE), jnp.bfloat16),
            jax.ShapeDtypeStruct((4, 4, 8, 1, 128), jnp.int32),
        ],
        in_specs=[hbm] * 4,
        out_specs=[hbm] * 4,
        scratch_shapes=[dma((4,))] + [dma((8,))] * 8 + [dma((40,))] * 2 + [dma((7,))] * 2,
        compiler_params=pltpu.CompilerParams(collective_id=0, has_side_effects=True, vmem_limit_bytes=2 * 2**20),
    )(queries, key_rows, value_matrix, docs)
    attended = attend(q, k, v, d)
    return pl.pallas_call(
        return_kernel,
        name="give_back",
        out_shape=jax.ShapeDtypeStruct((rows, 8 * WIDE), jnp.bfloat16),
        in_specs=[hbm],
        out_specs=hbm,
        scratch_shapes=[dma(()), dma((8,)), dma((8,))],
        compiler_params=pltpu.CompilerParams(collective_id=1, has_side_effects=True, vmem_limit_bytes=2 * 2**20),
    )(attended)


def solution(mesh):
    tokens = ("kv", "head")
    return jax.shard_map(
        local,
        mesh=mesh,
        in_specs=(P(tokens, None), P(tokens, None), P(tokens, None), P(tokens)),
        out_specs=P(tokens, None),
        check_vma=False,
    )
```
